32 devices in a mesh: grp: 2 (over y), row: 16 (over z, x, core).
Axes of the slice: x: 2, y: 2, z: 4, core: 2. Of those that a mesh axis runs over, the one named last changes fastest.
Arguments:
- right_side: float32 [64, 4096], P(None, ('grp', 'row')), may hold values from -60 to 60
- links: int32 [8, 4096], P(None, ('grp', 'row')), may hold values from 0 to 4095, as said below
- coefs: float32 [4096], P(('grp', 'row')), may hold values from 0.3 to 3
- reaction: float32 [4096], P(('grp', 'row')), may hold values from 0.05 to 0.5
Outputs:
- solution: float32 [64, 4096], P(None, ('grp', 'row'))
- resid_rms: float32 [2, 64], replicated
The draws below stay inside these ranges and needn't reach their ends.
Inputs may be any that keep to these rules, and one draw needn't show every extreme that they name: `links`: the nodes form a periodic grid of 8 x 32 x 16. Block (p, q), p < 2, q < 16, holds the nodes of first coordinate p * 4 to p * 4 + 3 and second coordinate q * 2 to q * 2 + 1, and these carry the unknowns and elements b * 4 * 2 * 16 to (b + 1) * 4 * 2 * 16 - 1, with b = p * 16 + q. Element b * 4 * 2 * 16 + (i * 2 + j) * 16 + k has its base at the node (p * 4 + i, q * 2 + j, k), and its corner l lies at the base plus (l mod 2, l // 2 mod 2, l // 4), modulo the grid. Within a block the unknowns are numbered in some order. Every unknown is a corner of 8 elements.
All inputs are finite; a program needn't handle non-finite values.
Results may differ from the reference program's by a relative error of at most 0.0003.
Values sent between devices are 32-bit elements; how exact they have to be, the bound alone decides.
A program may use at most 64 MiB of HBM per device.

```python
import math
import jax
import jax.numpy as jnp
import numpy as np
from jax import lax

CX = 4
CY = 2
CZ = 16
NRHS = 64
SWEEPS = 2
DEGREE = 4
NX = 8
NY = 32
NDOF = 4096
ELEMS = 4096


def draw_right_side(key, part):
    key_noise = jax.random.fold_in(key, 11)
    block_size = CX * CY * CZ
    block_count = NDOF // block_size
    position = (jnp.arange(NDOF) // block_size).astype(jnp.float32)
    rising = 1.0 + 2.0 * position / max(block_count - 1, 1)
    noise = jnp.clip(jax.random.normal(key_noise, (NRHS, NDOF), jnp.float32), -5.0, 5.0)
    return noise * rising


def draw_links(key, part):
    block_size = CX * CY * CZ
    block_count = NDOF // block_size
    row_blocks = NY // CY
    block_keys = jax.vmap(lambda number: jax.random.fold_in(key, number))(jnp.arange(block_count))
    orders = jax.vmap(lambda subkey: jax.random.permutation(subkey, block_size))(block_keys)
    element = jnp.arange(NDOF)
    owner = element // block_size
    inside = element % block_size
    first_block = owner // row_blocks
    second_block = owner % row_blocks
    first_pos = inside // (CY * CZ)
    second_pos = inside // CZ % CY
    third_pos = inside % CZ
    columns = []
    for corner in range(8):
        first = (first_block * CX + first_pos + corner % 2) % NX
        second = (second_block * CY + second_pos + corner // 2 % 2) % NY
        third = (third_pos + corner // 4) % CZ
        target = first // CX * row_blocks + second // CY
        spot = (first % CX * CY + second % CY) * CZ + third
        columns.append(target * block_size + orders[target, spot])
    return jnp.stack(columns, axis=0).astype(jnp.int32)


def levels(own_key, extent, cuts, least, top_value):
    def one(dim, parts):
        heights = jax.random.uniform(jax.random.fold_in(jax.random.fold_in(own_key, 6), dim), (parts,), jnp.float32, least / len(cuts), top_value / len(cuts))
        return jnp.repeat(jnp.exp(heights), extent[dim] // parts).reshape((-1,) + (1,) * (len(extent) - dim - 1))

    loudness = one(*cuts[0])
    for cut in cuts[1:]:
        loudness = loudness * one(*cut)
    return loudness


def setup_inputs(seed: int = 0) -> dict:
    streams_of = jax.random.split(jax.random.key(seed), 5)
    return {
        "right_side": draw_right_side(jax.random.fold_in(streams_of[4], 71), 0),
        "links": draw_links(jax.random.fold_in(streams_of[4], 71), 0),
        "coefs": jnp.clip(jnp.exp(math.log(3.0) - 2.3025851 * jax.random.uniform(streams_of[2], (ELEMS,), jnp.float32) ** levels(streams_of[2], (ELEMS,), ((0, 32),), -0.2, 0.2)), 0.3, 3.0),
        "reaction": jnp.clip(jnp.exp(math.log(0.5) - 2.3025851 * jax.random.uniform(streams_of[3], (NDOF,), jnp.float32) ** levels(streams_of[3], (NDOF,), ((0, 32),), -0.2, 0.2)), 0.05, 0.5),
    }


def element_matrix():
    node_ids = np.arange(8)
    corner = np.stack([node_ids % 2, node_ids // 2 % 2, node_ids // 4], axis=1)
    gauss_points = np.array([0.5 - 0.5 / math.sqrt(3.0), 0.5 + 0.5 / math.sqrt(3.0)])
    stiffness = np.zeros((8, 8))
    for q in range(8):
        quad_point = gauss_points[np.array([q % 2, q // 2 % 2, q // 4])]
        values = np.where(corner > 0.5, quad_point, 1.0 - quad_point)
        slopes = np.where(corner > 0.5, 1.0, -1.0)
        gradient = np.stack([slopes[:, 0] * values[:, 1] * values[:, 2], values[:, 0] * slopes[:, 1] * values[:, 2], values[:, 0] * values[:, 1] * slopes[:, 2]], axis=1)
        stiffness = stiffness + gradient @ gradient.T / 8.0
    return stiffness

def apply_operator(field, links, coefs, reaction, stiffness):
    corners = field[:, links]
    images = jnp.einsum('ml,rle->rme', stiffness, corners, precision=lax.Precision.HIGHEST) * coefs
    result = reaction * field
    return result.at[:, links].add(images)

def reference(right_side, links, coefs, reaction):
    stiffness = jnp.asarray(element_matrix(), dtype=jnp.float32)
    image = apply_operator(right_side, links, coefs, reaction, stiffness)
    theta = lax.optimization_barrier(jnp.sum(image * image, axis=1)) / lax.optimization_barrier(jnp.sum(right_side * image, axis=1))
    upper = (1.5 * theta)[:, None]
    lower = upper / 10.0
    center = (upper + lower) / 2.0
    half = (upper - lower) / 2.0
    sigma = center / half
    solution = jnp.zeros_like(right_side)
    residual = right_side
    history = []
    for sweep in range(SWEEPS):
        start = residual
        correction = jnp.zeros_like(right_side)
        rho_now = 1.0 / sigma
        direction = residual / center
        for step in range(DEGREE):
            correction = correction + direction
            residual = residual - apply_operator(direction, links, coefs, reaction, stiffness)
            if step + 1 < DEGREE:
                rho_next = 1.0 / (2.0 * sigma - rho_now)
                direction = rho_next * rho_now * direction + 2.0 * rho_next / half * residual
                rho_now = rho_next
        change = start - residual
        omega = (lax.optimization_barrier(jnp.sum(start * change, axis=1)) / lax.optimization_barrier(jnp.sum(change * change, axis=1)))[:, None]
        solution = solution + omega * correction
        residual = start - omega * change
        history.append(jnp.sqrt(lax.optimization_barrier(jnp.sum(residual * residual, axis=1)) / NDOF))
    return (solution, jnp.stack(history, axis=0))
```

```python
import functools
import math

import jax
import jax.numpy as jnp
import numpy as np
from jax import lax
from jax.experimental import pallas as pl
from jax.experimental.pallas import tpu as pltpu
from jax.sharding import PartitionSpec as P

SWEEPS = 2
DEGREE = 4
CX, CY, CZ = 4, 2, 16
SUB, LANES = 8, 128
MESH = pl.DeviceIdType.MESH
HIGHEST = lax.Precision.HIGHEST


def shifted(block, axis, distance):
    devices = range(lax.axis_size(axis))
    route = [((i - distance) % len(devices), i) for i in devices]
    return lax.ppermute(block, axis, route)


def element_matrix():
    node_ids = np.arange(8)
    corner = np.stack([node_ids % 2, node_ids // 2 % 2, node_ids // 4], axis=1)
    gauss_points = np.array([0.5 - 0.5 / math.sqrt(3.0), 0.5 + 0.5 / math.sqrt(3.0)])
    stiffness = np.zeros((8, 8))
    for q in range(8):
        quad_point = gauss_points[np.array([q % 2, q // 2 % 2, q // 4])]
        values = np.where(corner > 0.5, quad_point, 1.0 - quad_point)
        slopes = np.where(corner > 0.5, 1.0, -1.0)
        gradient = np.stack(
            [
                slopes[:, 0] * values[:, 1] * values[:, 2],
                values[:, 0] * slopes[:, 1] * values[:, 2],
                values[:, 0] * values[:, 1] * slopes[:, 2],
            ],
            axis=1,
        )
        stiffness = stiffness + gradient @ gradient.T / 8.0
    return stiffness


def element_images(window, offsets, weights, stiffness):
    corners = window[:, offsets]
    images = (
        jnp.einsum("ml,rle->rme", stiffness, corners, precision=lax.Precision.HIGHEST) * weights
    )
    return jnp.zeros_like(window).at[:, offsets].add(images)


def on_device(right_side, links, coefs, reaction):
    stiffness = jnp.asarray(element_matrix(), dtype=jnp.float32)
    count = right_side.shape[1]
    groups = lax.axis_size("grp")
    rowcount = lax.axis_size("row")
    group_id = lax.axis_index("grp")
    row_id = lax.axis_index("row")
    total = count * groups * rowcount
    owner = links // count
    slot = links % count
    first = jnp.mod(owner // rowcount - group_id, groups)
    second = jnp.mod(owner % rowcount - row_id, rowcount)
    offsets = (first * 2 + second) * count + slot

    def apply_operator(field):
        above_row = shifted(field, "row", -1)
        upper = shifted(jnp.stack([field, above_row], axis=0), "grp", -1)
        window = jnp.concatenate([field, above_row, upper[0], upper[1]], axis=1)
        summed = element_images(window, offsets, coefs, stiffness)
        back = shifted(
            jnp.stack([summed[:, 2 * count : 3 * count], summed[:, 3 * count :]], axis=0), "grp", 1
        )
        first_col = summed[:, :count] + back[0]
        second_col = summed[:, count : 2 * count] + back[1]
        first_col = first_col + shifted(second_col, "row", 1)
        return first_col + reaction * field

    image = apply_operator(right_side)
    cross, square = lax.psum(
        (jnp.sum(right_side * image, axis=1), jnp.sum(image * image, axis=1)), ("grp", "row")
    )
    theta = square / cross
    upper = (1.5 * theta)[:, None]
    lower = upper / 10.0
    center = (upper + lower) / 2.0
    half = (upper - lower) / 2.0
    sigma = center / half
    solution = jnp.zeros_like(right_side)
    residual = right_side
    history = []
    for sweep in range(SWEEPS):
        start = residual
        correction = jnp.zeros_like(right_side)
        rho_now = 1.0 / sigma
        direction = residual / center
        for step in range(DEGREE):
            correction = correction + direction
            residual = residual - apply_operator(direction)
            if step + 1 < DEGREE:
                rho_next = 1.0 / (2.0 * sigma - rho_now)
                direction = rho_next * rho_now * direction + 2.0 * rho_next / half * residual
                rho_now = rho_next
        change = start - residual
        along, length, begin = lax.psum(
            (
                jnp.sum(start * change, axis=1),
                jnp.sum(change * change, axis=1),
                jnp.sum(start * start, axis=1),
            ),
            ("grp", "row"),
        )
        omega = along / length
        residual = start - omega[:, None] * change
        squares = begin - 2.0 * omega * along + omega * omega * length
        solution = solution + omega[:, None] * correction
        history.append(jnp.sqrt(squares / total))
    return (solution, jnp.stack(history, axis=0))


def next_x(plane):
    return jnp.concatenate([plane[1:], plane[:1]], axis=0)


def last_x(plane):
    return jnp.concatenate([plane[-1:], plane[:-1]], axis=0)


def next_z(plane):
    turned = pltpu.roll(plane, SUB - 1, 1)
    place = lax.broadcasted_iota(jnp.int32, plane.shape, 1)
    return jnp.where(place == SUB - 1, pltpu.roll(turned, LANES // 2, 2), turned)


def last_z(plane):
    turned = pltpu.roll(plane, 1, 1)
    place = lax.broadcasted_iota(jnp.int32, plane.shape, 1)
    return jnp.where(place == 0, pltpu.roll(turned, LANES // 2, 2), turned)


def chebyshev_weights(theta):
    upper = 1.5 * theta
    lower = upper / 10.0
    center = (upper + lower) / 2.0
    half = (upper - lower) / 2.0
    sigma = center / half
    rho_now = 1.0 / sigma
    direction = [1.0 / center]
    residual = [jnp.ones_like(theta)]
    correction = []
    for step in range(DEGREE):
        size = len(direction)
        correction = [
            direction[k] + correction[k] if k < len(correction) else direction[k]
            for k in range(size)
        ]
        residual = [residual[0]] + [
            residual[k] - direction[k - 1] if k < len(residual) else -direction[k - 1]
            for k in range(1, size + 1)
        ]
        if step + 1 < DEGREE:
            rho_next = 1.0 / (2.0 * sigma - rho_now)
            direction = [
                rho_next * rho_now * direction[k] + 2.0 * rho_next / half * residual[k]
                if k < size
                else 2.0 * rho_next / half * residual[k]
                for k in range(size + 1)
            ]
            rho_now = rho_next
    return correction, [-value for value in residual[1:]]


def kernel(
    groups, rowcount, total,
    right_ref, links_ref, coefs_ref, react_ref,
    out_ref, rms_ref,
    field, mass, diag, edge_x, edge_y, edge_z, aux,
    power1, power2, power3, power4, moved, sums,
    field_send, field_recv, aux_send, aux_recv, moved_send, moved_recv, sums_send, sums_recv,
):
    reach = DEGREE // CY
    grp = lax.axis_index("grp")
    row = lax.axis_index("row")
    own = range(reach * CY, reach * CY + CY)
    nrhs = right_ref.shape[0]
    count = right_ref.shape[1]

    def row_at(offset):
        return lax.rem(row + offset + rowcount, rowcount)

    near = [(o, d) for o in sorted(range(-reach, reach + 1), key=lambda o: -abs(o)) for d in range(groups)]
    near = [(o, d) for o, d in near if o or d]

    barrier = pltpu.get_barrier_semaphore()
    greeted = 0
    for o in range(1, rowcount):
        pl.semaphore_signal(barrier, inc=1, device_id=(grp, row_at(o)), device_id_type=MESH)
        greeted += 1
    for o, d in near:
        if d:
            peer = (lax.rem(grp + d, groups), row_at(o))
            pl.semaphore_signal(barrier, inc=1, device_id=peer, device_id_type=MESH)
            greeted += 1

    home = (grp * rowcount + row) * count
    slots = jnp.broadcast_to(links_ref[0:1, :] - home, (count, count))
    slot_of = (slots == lax.broadcasted_iota(jnp.int32, (count, count), 0)).astype(jnp.float32)
    order = jnp.transpose(slot_of)
    lanes = lax.broadcasted_iota(jnp.int32, (CX, SUB, LANES), 2)
    low = lanes < LANES // 2
    react = jnp.dot(
        jnp.broadcast_to(react_ref[...], (SUB, count)), slot_of,
        precision=HIGHEST, preferred_element_type=jnp.float32,
    )
    which = lax.broadcasted_iota(jnp.int32, (SUB, count), 0)
    my_aux = reach * groups + grp
    aux[my_aux] = jnp.where(
        which == 0, jnp.broadcast_to(coefs_ref[...], (SUB, count)) * (1.0 / 12.0), react
    )
    twice = jnp.concatenate([right_ref[...], right_ref[...]], axis=0)
    nodes = lax.dot_general(
        order, twice, (((1,), (1,)), ((), ())), precision=HIGHEST,
        preferred_element_type=jnp.float32,
    ).reshape(CX, CY, 2, SUB, LANES)
    for y in range(CY):
        field[reach * CY + y, pl.ds(grp * CX, CX)] = jnp.where(low, nodes[:, y, 0], nodes[:, y, 1])

    pl.semaphore_wait(barrier, greeted)
    aux_copies, field_copies = [], []
    for k, (o, d) in enumerate(near):
        peer = (lax.rem(grp + d, groups), row_at(o))
        copy = pltpu.make_async_remote_copy(
            src_ref=aux.at[my_aux], dst_ref=aux.at[(reach - o) * groups + grp],
            send_sem=aux_send.at[k], recv_sem=aux_recv.at[k], device_id=peer, device_id_type=MESH,
        )
        copy.start()
        aux_copies.append(copy)
    for k, (o, d) in enumerate(near):
        peer = (lax.rem(grp + d, groups), row_at(o))
        copy = pltpu.make_async_remote_copy(
            src_ref=field.at[pl.ds(reach * CY, CY), pl.ds(grp * CX, CX)],
            dst_ref=field.at[pl.ds((reach - o) * CY, CY), pl.ds(grp * CX, CX)],
            send_sem=field_send.at[k], recv_sem=field_recv.at[k], device_id=peer, device_id_type=MESH,
        )
        copy.start()
        field_copies.append(copy)

    for copy in aux_copies:
        copy.wait_recv()
    blocks = 2 * reach + 1
    table = aux[...].reshape(blocks * groups * SUB, count)
    table = jnp.concatenate([table, jnp.zeros((count - table.shape[0], count), jnp.float32)], axis=0)
    columns = jnp.transpose(table).reshape(CX, CY, 2, SUB, LANES)
    for b in range(blocks):
        for g in range(groups):
            for y in range(CY):
                for entry, target in ((0, mass), (1, diag)):
                    at = (b * groups + g) * SUB + entry
                    first = jnp.broadcast_to(columns[:, y, 0, :, at : at + 1], (CX, SUB, LANES))
                    second = jnp.broadcast_to(columns[:, y, 1, :, at : at + 1], (CX, SUB, LANES))
                    target[b * CY + y, g * CX : (g + 1) * CX] = jnp.where(low, first, second)
    planes = blocks * CY
    before_xz = before_x = before_z = before = None
    for y in range(planes - 1):
        here = mass[y]
        here_z = here + last_z(here)
        here_x = here + last_x(here)
        here_xz = here_z + last_x(here_z)
        edge_y[y] = here_xz
        if y:
            edge_x[y] = here_z + before_z
            edge_z[y] = here_x + before_x
            diag[y] = diag[y] + 5.0 * (here_xz + before_xz)
        before_xz, before_x, before_z = here_xz, here_x, here_z

    def apply_operator(source, target, begin, end):
        def gathered(y):
            value = source[y]
            above = next_z(value)
            pair = value + above
            return value, above, pair + next_x(pair)

        last, _, last_sum = gathered(begin - 1)
        value, above, here_sum = gathered(begin)
        last_push = mass[begin - 1] * (last_sum + here_sum)
        for y in range(begin, end):
            following, following_above, following_sum = gathered(y + 1)
            push = mass[y] * (here_sum + following_sum)
            push_y = push + last_push
            push_x = push_y + last_x(push_y)
            result = diag[y] * value - push_x + edge_z[y] * above
            result = result + edge_x[y] * next_x(value) + last_x(edge_x[y] * value)
            result = result + edge_y[y] * following + edge_y[y - 1] * last
            target[y] = result + last_z(edge_z[y] * value - push_x)
            last, last_push = value, push
            value, above, here_sum = following, following_above, following_sum

    def across(products):
        return jnp.sum(jnp.sum(products, axis=0), axis=0, keepdims=True)

    def start_sum(number, rows):
        rows = rows + [jnp.zeros_like(rows[0])] * (sums.shape[2] - len(rows))
        sums[number, row] = jnp.concatenate(rows, axis=0)
        copies = []
        for o in range(1, rowcount):
            copy = pltpu.make_async_remote_copy(
                src_ref=sums.at[number, row], dst_ref=sums.at[number, row],
                send_sem=sums_send.at[number, o - 1], recv_sem=sums_recv.at[number, o - 1],
                device_id=(grp, row_at(o)), device_id_type=MESH,
            )
            copy.start()
            copies.append(copy)
        return copies

    def end_sum(number, copies):
        for copy in copies:
            copy.wait_recv()
        added = jnp.sum(sums[number], axis=0)
        return added + pltpu.roll(added, LANES // 2, 1)

    def spread(line):
        return jnp.broadcast_to(line, (SUB, LANES))

    def combined(weights, powers, y):
        value = weights[0] * powers[0][y]
        for weight, power in zip(weights[1:], powers[1:]):
            value = value + weight * power[y]
        return value

    for copy in field_copies:
        copy.wait_recv()
    first, final = reach * CY, reach * CY + CY
    apply_operator(field, power1, first, final)
    cross = sum(across(field[y] * power1[y]) for y in own)
    square = sum(across(power1[y] * power1[y]) for y in own)
    begin = sum(across(field[y] * field[y]) for y in own)
    bound = start_sum(0, [cross, square, begin])
    apply_operator(field, power1, 1, first)
    apply_operator(field, power1, final, planes - 1)
    apply_operator(power1, power2, 2, planes - 2)
    apply_operator(power2, power3, 3, planes - 3)
    apply_operator(power3, power4, 4, planes - 4)
    powers = [field, power1, power2, power3, power4]
    added = end_sum(0, bound)
    correct, differ = chebyshev_weights(spread(added[1:2] / added[0:1]))
    begin = spread(added[2:3])

    for y in own:
        moved[y] = combined(differ, powers[1:], y)
    moved_copies = []
    for k, o in enumerate(o for o in range(-reach, reach + 1) if o):
        copy = pltpu.make_async_remote_copy(
            src_ref=moved.at[pl.ds(reach * CY, CY)], dst_ref=moved.at[pl.ds((reach - o) * CY, CY)],
            send_sem=moved_send.at[k], recv_sem=moved_recv.at[k],
            device_id=(grp, row_at(o)), device_id_type=MESH,
        )
        copy.start()
        moved_copies.append(copy)
    along = sum(across(field[y] * moved[y]) for y in own)
    length = sum(across(moved[y] * moved[y]) for y in own)
    step_sum = start_sum(1, [along, length])

    half_rows = [order.reshape(CX, CY, 2, SUB, count)[:, :, z] for z in range(2)]
    half_rows = [
        jnp.concatenate([part[:, y].reshape(CX * SUB, count) for y in range(CY)], axis=0)
        for part in half_rows
    ]

    def mine(y, value):
        return jnp.where(grp == 0, value[:CX], value[CX:])

    def to_slots(parts):
        stacked = jnp.concatenate([part.reshape(CX * SUB, LANES) for part in parts], axis=0)
        turned = jnp.transpose(stacked)
        return sum(
            jnp.dot(
                turned[z * nrhs : (z + 1) * nrhs], half_rows[z],
                precision=HIGHEST, preferred_element_type=jnp.float32,
            )
            for z in range(2)
        )

    corrections = [mine(y, combined(correct, powers[:-1], y)) for y in own]

    def rms(omega, along, length, begin):
        squares = begin - 2.0 * omega * along + omega * omega * length
        return jnp.sqrt(squares / total)

    added = end_sum(1, step_sum)
    along, length = spread(added[0:1]), spread(added[1:2])
    omega = along / length
    first_rms = rms(omega, along, length, begin)
    corrections = [omega * part for part in corrections]
    for copy in moved_copies:
        copy.wait_recv()
    for copy in field_copies:
        copy.wait_send()
    for y in range(planes):
        field[y] = field[y] - omega * moved[y]
    apply_operator(field, power1, 1, planes - 1)
    apply_operator(power1, power2, 2, planes - 2)
    apply_operator(power2, power3, 3, planes - 3)
    apply_operator(power3, power4, 4, planes - 4)
    along = length = begin = 0.0
    for y in own:
        change = combined(differ, powers[1:], y)
        along = along + across(field[y] * change)
        length = length + across(change * change)
        begin = begin + across(field[y] * field[y])
    step_sum = start_sum(2, [along, length, begin])
    settled = to_slots(corrections)
    later = to_slots([mine(y, combined(correct, powers[:-1], y)) for y in own])
    added = end_sum(2, step_sum)
    along, length, begin = (spread(added[k : k + 1]) for k in range(3))
    omega = along / length
    second_rms = rms(omega, along, length, begin)
    rms_ref[...] = jnp.concatenate([first_rms[0:1, :nrhs], second_rms[0:1, :nrhs]], axis=0)
    column = jnp.transpose(jnp.broadcast_to(omega[0:1], (LANES, LANES)))[:nrhs]
    out_ref[...] = settled + column * later
    for copy in aux_copies + moved_copies + bound:
        copy.wait_send()
    for o in range(1, rowcount):
        for number in range(1, 3):
            pltpu.make_async_remote_copy(
                src_ref=sums.at[number, row], dst_ref=sums.at[number, row],
                send_sem=sums_send.at[number, o - 1], recv_sem=sums_recv.at[number, o - 1],
                device_id=(grp, row_at(o)), device_id_type=MESH,
            ).wait_send()


def whole_sweeps(groups, rowcount, right_side, links, coefs, reaction):
    nrhs, count = right_side.shape
    reach = DEGREE // CY
    planes = (2 * reach + 1) * CY
    window = pltpu.VMEM((planes, groups * CX, SUB, LANES), jnp.float32)
    nears = groups * (2 * reach + 1) - 1
    dma = pltpu.SemaphoreType.DMA
    vmem = pl.BlockSpec(memory_space=pltpu.VMEM)
    return pl.pallas_call(
        functools.partial(kernel, groups, rowcount, count * groups * rowcount),
        out_shape=(
            jax.ShapeDtypeStruct((nrhs, count), jnp.float32),
            jax.ShapeDtypeStruct((SWEEPS, nrhs), jnp.float32),
        ),
        in_specs=[vmem] * 4,
        out_specs=(vmem, vmem),
        scratch_shapes=[
            window, window, window, window, window, window,
            pltpu.VMEM(((2 * reach + 1) * groups, SUB, count), jnp.float32),
            window, window, window, window, window,
            pltpu.VMEM((3, rowcount, 4, LANES), jnp.float32),
            dma((nears,)), dma((nears,)), dma((nears,)), dma((nears,)),
            dma((2 * reach,)), dma((2 * reach,)),
            dma((3, rowcount - 1)), dma((3, rowcount - 1)),
        ],
        compiler_params=pltpu.CompilerParams(collective_id=0, has_side_effects=True),
    )(right_side, links, coefs.reshape(1, count), reaction.reshape(1, count))


def in_one_kernel(mesh):
    return mesh.shape["grp"] == 2 and mesh.shape["row"] >= 2 * (DEGREE // CY) + 1


def solution(mesh):
    body = on_device
    if in_one_kernel(mesh):
        body = functools.partial(whole_sweeps, mesh.shape["grp"], mesh.shape["row"])
    return jax.shard_map(
        body,
        mesh=mesh,
        in_specs=(
            P(None, ("grp", "row")),
            P(None, ("grp", "row")),
            P(("grp", "row")),
            P(("grp", "row")),
        ),
        out_specs=(P(None, ("grp", "row")), P()),
        check_vma=False,
    )
```

```python
import functools
import math

import jax
import jax.numpy as jnp
import numpy as np
from jax import lax
from jax.experimental import pallas as pl
from jax.experimental.pallas import tpu as pltpu
from jax.sharding import PartitionSpec as P

SWEEPS = 2
DEGREE = 4
CX, CY, CZ = 4, 2, 16
SUB, LANES = 8, 128
MESH = pl.DeviceIdType.MESH
HIGHEST = lax.Precision.HIGHEST


def shifted(block, axis, distance):
    devices = range(lax.axis_size(axis))
    route = [((i - distance) % len(devices), i) for i in devices]
    return lax.ppermute(block, axis, route)


def element_matrix():
    node_ids = np.arange(8)
    corner = np.stack([node_ids % 2, node_ids // 2 % 2, node_ids // 4], axis=1)
    gauss_points = np.array([0.5 - 0.5 / math.sqrt(3.0), 0.5 + 0.5 / math.sqrt(3.0)])
    stiffness = np.zeros((8, 8))
    for q in range(8):
        quad_point = gauss_points[np.array([q % 2, q // 2 % 2, q // 4])]
        values = np.where(corner > 0.5, quad_point, 1.0 - quad_point)
        slopes = np.where(corner > 0.5, 1.0, -1.0)
        gradient = np.stack(
            [
                slopes[:, 0] * values[:, 1] * values[:, 2],
                values[:, 0] * slopes[:, 1] * values[:, 2],
                values[:, 0] * values[:, 1] * slopes[:, 2],
            ],
            axis=1,
        )
        stiffness = stiffness + gradient @ gradient.T / 8.0
    return stiffness


def element_images(window, offsets, weights, stiffness):
    corners = window[:, offsets]
    images = (
        jnp.einsum("ml,rle->rme", stiffness, corners, precision=lax.Precision.HIGHEST) * weights
    )
    return jnp.zeros_like(window).at[:, offsets].add(images)


def on_device(right_side, links, coefs, reaction):
    stiffness = jnp.asarray(element_matrix(), dtype=jnp.float32)
    count = right_side.shape[1]
    groups = lax.axis_size("grp")
    rowcount = lax.axis_size("row")
    group_id = lax.axis_index("grp")
    row_id = lax.axis_index("row")
    total = count * groups * rowcount
    owner = links // count
    slot = links % count
    first = jnp.mod(owner // rowcount - group_id, groups)
    second = jnp.mod(owner % rowcount - row_id, rowcount)
    offsets = (first * 2 + second) * count + slot

    def apply_operator(field):
        above_row = shifted(field, "row", -1)
        upper = shifted(jnp.stack([field, above_row], axis=0), "grp", -1)
        window = jnp.concatenate([field, above_row, upper[0], upper[1]], axis=1)
        summed = element_images(window, offsets, coefs, stiffness)
        back = shifted(
            jnp.stack([summed[:, 2 * count : 3 * count], summed[:, 3 * count :]], axis=0), "grp", 1
        )
        first_col = summed[:, :count] + back[0]
        second_col = summed[:, count : 2 * count] + back[1]
        first_col = first_col + shifted(second_col, "row", 1)
        return first_col + reaction * field

    image = apply_operator(right_side)
    cross, square = lax.psum(
        (jnp.sum(right_side * image, axis=1), jnp.sum(image * image, axis=1)), ("grp", "row")
    )
    theta = square / cross
    upper = (1.5 * theta)[:, None]
    lower = upper / 10.0
    center = (upper + lower) / 2.0
    half = (upper - lower) / 2.0
    sigma = center / half
    solution = jnp.zeros_like(right_side)
    residual = right_side
    history = []
    for sweep in range(SWEEPS):
        start = residual
        correction = jnp.zeros_like(right_side)
        rho_now = 1.0 / sigma
        direction = residual / center
        for step in range(DEGREE):
            correction = correction + direction
            residual = residual - apply_operator(direction)
            if step + 1 < DEGREE:
                rho_next = 1.0 / (2.0 * sigma - rho_now)
                direction = rho_next * rho_now * direction + 2.0 * rho_next / half * residual
                rho_now = rho_next
        change = start - residual
        along, length, begin = lax.psum(
            (
                jnp.sum(start * change, axis=1),
                jnp.sum(change * change, axis=1),
                jnp.sum(start * start, axis=1),
            ),
            ("grp", "row"),
        )
        omega = along / length
        residual = start - omega[:, None] * change
        squares = begin - 2.0 * omega * along + omega * omega * length
        solution = solution + omega[:, None] * correction
        history.append(jnp.sqrt(squares / total))
    return (solution, jnp.stack(history, axis=0))


def next_x(plane):
    return jnp.concatenate([plane[1:], plane[:1]], axis=0)


def last_x(plane):
    return jnp.concatenate([plane[-1:], plane[:-1]], axis=0)


def next_z(plane):
    turned = pltpu.roll(plane, SUB - 1, 1)
    place = lax.broadcasted_iota(jnp.int32, plane.shape, 1)
    return jnp.where(place == SUB - 1, pltpu.roll(turned, LANES // 2, 2), turned)


def last_z(plane):
    turned = pltpu.roll(plane, 1, 1)
    place = lax.broadcasted_iota(jnp.int32, plane.shape, 1)
    return jnp.where(place == 0, pltpu.roll(turned, LANES // 2, 2), turned)


def chebyshev_weights(theta):
    upper = 1.5 * theta
    lower = upper / 10.0
    center = (upper + lower) / 2.0
    half = (upper - lower) / 2.0
    sigma = center / half
    rho_now = 1.0 / sigma
    direction = [1.0 / center]
    residual = [jnp.ones_like(theta)]
    correction = []
    for step in range(DEGREE):
        size = len(direction)
        correction = [
            direction[k] + correction[k] if k < len(correction) else direction[k]
            for k in range(size)
        ]
        residual = [residual[0]] + [
            residual[k] - direction[k - 1] if k < len(residual) else -direction[k - 1]
            for k in range(1, size + 1)
        ]
        if step + 1 < DEGREE:
            rho_next = 1.0 / (2.0 * sigma - rho_now)
            direction = [
                rho_next * rho_now * direction[k] + 2.0 * rho_next / half * residual[k]
                if k < size
                else 2.0 * rho_next / half * residual[k]
                for k in range(size + 1)
            ]
            rho_now = rho_next
    return correction, [-value for value in residual[1:]]


def kernel(
    groups, rowcount, total,
    right_ref, links_ref, coefs_ref, react_ref,
    packed_ref,
    field, mass, diag, edge_x, edge_y, edge_z, aux,
    power1, power2, power3, power4, moved, sums,
    field_send, field_recv, aux_send, aux_recv, moved_send, moved_recv, sums_send, sums_recv,
):
    reach = DEGREE // CY
    grp = lax.axis_index("grp")
    row = lax.axis_index("row")
    own = range(reach * CY, reach * CY + CY)
    nrhs = right_ref.shape[0]
    count = right_ref.shape[1]

    def row_at(offset):
        return lax.rem(row + offset + rowcount, rowcount)

    near = [(o, d) for o in sorted(range(-reach, reach + 1), key=lambda o: -abs(o)) for d in range(groups)]
    near = [(o, d) for o, d in near if o or d]

    barrier = pltpu.get_barrier_semaphore()
    greeted = 0
    for o in range(1, rowcount):
        pl.semaphore_signal(barrier, inc=1, device_id=(grp, row_at(o)), device_id_type=MESH)
        greeted += 1
    for o, d in near:
        if d:
            peer = (lax.rem(grp + d, groups), row_at(o))
            pl.semaphore_signal(barrier, inc=1, device_id=peer, device_id_type=MESH)
            greeted += 1

    home = (grp * rowcount + row) * count
    slots = jnp.broadcast_to(links_ref[0:1, :] - home, (count, count))
    slot_of = (slots == lax.broadcasted_iota(jnp.int32, (count, count), 0)).astype(jnp.float32)
    order = jnp.transpose(slot_of)
    lanes = lax.broadcasted_iota(jnp.int32, (CX, SUB, LANES), 2)
    low = lanes < LANES // 2
    react = jnp.dot(
        jnp.broadcast_to(react_ref[...], (SUB, count)), slot_of,
        precision=HIGHEST, preferred_element_type=jnp.float32,
    )
    which = lax.broadcasted_iota(jnp.int32, (SUB, count), 0)
    my_aux = reach * groups + grp
    aux[my_aux] = jnp.where(
        which == 0, jnp.broadcast_to(coefs_ref[...], (SUB, count)) * (1.0 / 12.0), react
    )
    twice = jnp.concatenate([right_ref[...], right_ref[...]], axis=0)
    nodes = lax.dot_general(
        order, twice, (((1,), (1,)), ((), ())), precision=HIGHEST,
        preferred_element_type=jnp.float32,
    ).reshape(CX, CY, 2, SUB, LANES)
    for y in range(CY):
        field[reach * CY + y, pl.ds(grp * CX, CX)] = jnp.where(low, nodes[:, y, 0], nodes[:, y, 1])

    pl.semaphore_wait(barrier, greeted)
    aux_copies, field_copies = [], []
    for k, (o, d) in enumerate(near):
        peer = (lax.rem(grp + d, groups), row_at(o))
        copy = pltpu.make_async_remote_copy(
            src_ref=aux.at[my_aux], dst_ref=aux.at[(reach - o) * groups + grp],
            send_sem=aux_send.at[k], recv_sem=aux_recv.at[k], device_id=peer, device_id_type=MESH,
        )
        copy.start()
        aux_copies.append(copy)
    for k, (o, d) in enumerate(near):
        peer = (lax.rem(grp + d, groups), row_at(o))
        copy = pltpu.make_async_remote_copy(
            src_ref=field.at[pl.ds(reach * CY, CY), pl.ds(grp * CX, CX)],
            dst_ref=field.at[pl.ds((reach - o) * CY, CY), pl.ds(grp * CX, CX)],
            send_sem=field_send.at[k], recv_sem=field_recv.at[k], device_id=peer, device_id_type=MESH,
        )
        copy.start()
        field_copies.append(copy)

    for copy in aux_copies:
        copy.wait_recv()
    blocks = 2 * reach + 1
    table = aux[...].reshape(blocks * groups * SUB, count)
    table = jnp.concatenate([table, jnp.zeros((count - table.shape[0], count), jnp.float32)], axis=0)
    columns = jnp.transpose(table).reshape(CX, CY, 2, SUB, LANES)
    for b in range(blocks):
        for g in range(groups):
            for y in range(CY):
                for entry, target in ((0, mass), (1, diag)):
                    at = (b * groups + g) * SUB + entry
                    first = jnp.broadcast_to(columns[:, y, 0, :, at : at + 1], (CX, SUB, LANES))
                    second = jnp.broadcast_to(columns[:, y, 1, :, at : at + 1], (CX, SUB, LANES))
                    target[b * CY + y, g * CX : (g + 1) * CX] = jnp.where(low, first, second)
    planes = blocks * CY
    before_xz = before_x = before_z = before = None
    for y in range(planes - 1):
        here = mass[y]
        here_z = here + last_z(here)
        here_x = here + last_x(here)
        here_xz = here_z + last_x(here_z)
        edge_y[y] = here_xz
        if y:
            edge_x[y] = here_z + before_z
            edge_z[y] = here_x + before_x
            diag[y] = diag[y] + 5.0 * (here_xz + before_xz)
        before_xz, before_x, before_z = here_xz, here_x, here_z

    def apply_operator(source, target, begin, end):
        def gathered(y):
            value = source[y]
            above = next_z(value)
            pair = value + above
            return value, above, pair + next_x(pair)

        last, _, last_sum = gathered(begin - 1)
        value, above, here_sum = gathered(begin)
        last_push = mass[begin - 1] * (last_sum + here_sum)
        for y in range(begin, end):
            following, following_above, following_sum = gathered(y + 1)
            push = mass[y] * (here_sum + following_sum)
            push_y = push + last_push
            push_x = push_y + last_x(push_y)
            result = diag[y] * value - push_x + edge_z[y] * above
            result = result + edge_x[y] * next_x(value) + last_x(edge_x[y] * value)
            result = result + edge_y[y] * following + edge_y[y - 1] * last
            target[y] = result + last_z(edge_z[y] * value - push_x)
            last, last_push = value, push
            value, above, here_sum = following, following_above, following_sum

    def across(products):
        return jnp.sum(jnp.sum(products, axis=0), axis=0, keepdims=True)

    def start_sum(number, rows):
        rows = rows + [jnp.zeros_like(rows[0])] * (sums.shape[2] - len(rows))
        sums[number, row] = jnp.concatenate(rows, axis=0)
        copies = []
        for o in sorted(range(1, rowcount), key=lambda o: -min(o, rowcount - o)):
            copy = pltpu.make_async_remote_copy(
                src_ref=sums.at[number, row], dst_ref=sums.at[number, row],
                send_sem=sums_send.at[number, o - 1], recv_sem=sums_recv.at[number, o - 1],
                device_id=(grp, row_at(o)), device_id_type=MESH,
            )
            copy.start()
            copies.append(copy)
        return copies

    def end_sum(number, copies):
        for copy in copies:
            copy.wait_recv()
        added = jnp.sum(sums[number], axis=0)
        return added + pltpu.roll(added, LANES // 2, 1)

    def spread(line):
        return jnp.broadcast_to(line, (SUB, LANES))

    def combined(weights, powers, y):
        value = weights[0] * powers[0][y]
        for weight, power in zip(weights[1:], powers[1:]):
            value = value + weight * power[y]
        return value

    for copy in field_copies:
        copy.wait_recv()
    first, final = reach * CY, reach * CY + CY
    apply_operator(field, power1, first, final)
    cross = sum(across(field[y] * power1[y]) for y in own)
    square = sum(across(power1[y] * power1[y]) for y in own)
    begin = sum(across(field[y] * field[y]) for y in own)
    bound = start_sum(0, [cross, square, begin])
    apply_operator(field, power1, 1, first)
    apply_operator(field, power1, final, planes - 1)
    apply_operator(power1, power2, 2, planes - 2)
    apply_operator(power2, power3, 3, planes - 3)
    apply_operator(power3, power4, 4, planes - 4)
    powers = [field, power1, power2, power3, power4]
    added = end_sum(0, bound)
    correct, differ = chebyshev_weights(spread(added[1:2] / added[0:1]))
    begin = spread(added[2:3])

    for y in own:
        moved[y] = combined(differ, powers[1:], y)
    moved_copies = []
    for k, o in enumerate(o for o in range(-reach, reach + 1) if o):
        copy = pltpu.make_async_remote_copy(
            src_ref=moved.at[pl.ds(reach * CY, CY)], dst_ref=moved.at[pl.ds((reach - o) * CY, CY)],
            send_sem=moved_send.at[k], recv_sem=moved_recv.at[k],
            device_id=(grp, row_at(o)), device_id_type=MESH,
        )
        copy.start()
        moved_copies.append(copy)
    along = sum(across(field[y] * moved[y]) for y in own)
    length = sum(across(moved[y] * moved[y]) for y in own)
    step_sum = start_sum(1, [along, length])

    half_rows = [order.reshape(CX, CY, 2, SUB, count)[:, :, z] for z in range(2)]
    half_rows = [
        jnp.concatenate([part[:, y].reshape(CX * SUB, count) for y in range(CY)], axis=0)
        for part in half_rows
    ]

    def mine(y, value):
        return jnp.where(grp == 0, value[:CX], value[CX:])

    def to_slots(parts):
        stacked = jnp.concatenate([part.reshape(CX * SUB, LANES) for part in parts], axis=0)
        turned = jnp.transpose(stacked)
        return sum(
            jnp.dot(
                turned[z * nrhs : (z + 1) * nrhs], half_rows[z],
                precision=HIGHEST, preferred_element_type=jnp.float32,
            )
            for z in range(2)
        )

    corrections = [mine(y, combined(correct, powers[:-1], y)) for y in own]

    def rms(omega, along, length, begin):
        squares = begin - 2.0 * omega * along + omega * omega * length
        return jnp.sqrt(squares / total)

    added = end_sum(1, step_sum)
    along, length = spread(added[0:1]), spread(added[1:2])
    omega = along / length
    first_rms = rms(omega, along, length, begin)
    corrections = [omega * part for part in corrections]
    for copy in moved_copies:
        copy.wait_recv()
    for copy in field_copies:
        copy.wait_send()
    for y in range(planes):
        field[y] = field[y] - omega * moved[y]
    apply_operator(field, power1, 1, planes - 1)
    apply_operator(power1, power2, 2, planes - 2)
    apply_operator(power2, power3, 3, planes - 3)
    apply_operator(power3, power4, 4, planes - 4)
    along = length = begin = 0.0
    for y in own:
        change = combined(differ, powers[1:], y)
        along = along + across(field[y] * change)
        length = length + across(change * change)
        begin = begin + across(field[y] * field[y])
    step_sum = start_sum(2, [along, length, begin])
    settled = to_slots(corrections)
    later = to_slots([mine(y, combined(correct, powers[:-1], y)) for y in own])
    added = end_sum(2, step_sum)
    along, length, begin = (spread(added[k : k + 1]) for k in range(3))
    omega = along / length
    second_rms = rms(omega, along, length, begin)
    packed_ref[pl.ds(nrhs, SUB)] = jnp.where(
        lax.broadcasted_iota(jnp.int32, (SUB, LANES), 0) == 0, first_rms, second_rms
    )
    column = jnp.transpose(jnp.broadcast_to(omega[0:1], (LANES, LANES)))[:nrhs]
    packed_ref[pl.ds(0, nrhs)] = settled + column * later
    for copy in aux_copies + moved_copies + bound:
        copy.wait_send()
    for o in range(1, rowcount):
        for number in range(1, 3):
            pltpu.make_async_remote_copy(
                src_ref=sums.at[number, row], dst_ref=sums.at[number, row],
                send_sem=sums_send.at[number, o - 1], recv_sem=sums_recv.at[number, o - 1],
                device_id=(grp, row_at(o)), device_id_type=MESH,
            ).wait_send()


def unpack(packed_ref, out_ref, rms_ref):
    nrhs = out_ref.shape[0]
    out_ref[...] = packed_ref[:nrhs]
    rms_ref[...] = packed_ref[nrhs : nrhs + SWEEPS, :nrhs]


def whole_sweeps(groups, rowcount, right_side, links, coefs, reaction):
    nrhs, count = right_side.shape
    reach = DEGREE // CY
    planes = (2 * reach + 1) * CY
    window = pltpu.VMEM((planes, groups * CX, SUB, LANES), jnp.float32)
    nears = groups * (2 * reach + 1) - 1
    dma = pltpu.SemaphoreType.DMA
    vmem = pl.BlockSpec(memory_space=pltpu.VMEM)
    packed = pl.pallas_call(
        functools.partial(kernel, groups, rowcount, count * groups * rowcount),
        out_shape=jax.ShapeDtypeStruct((nrhs + SUB, count), jnp.float32),
        in_specs=[vmem] * 4,
        out_specs=vmem,
        scratch_shapes=[
            window, window, window, window, window, window,
            pltpu.VMEM(((2 * reach + 1) * groups, SUB, count), jnp.float32),
            window, window, window, window, window,
            pltpu.VMEM((3, rowcount, 4, LANES), jnp.float32),
            dma((nears,)), dma((nears,)), dma((nears,)), dma((nears,)),
            dma((2 * reach,)), dma((2 * reach,)),
            dma((3, rowcount - 1)), dma((3, rowcount - 1)),
        ],
        compiler_params=pltpu.CompilerParams(collective_id=0, has_side_effects=True),
    )(right_side, links, coefs.reshape(1, count), reaction.reshape(1, count))
    return pl.pallas_call(
        unpack,
        out_shape=(
            jax.ShapeDtypeStruct((nrhs, count), jnp.float32),
            jax.ShapeDtypeStruct((SWEEPS, nrhs), jnp.float32),
        ),
        in_specs=[vmem],
        out_specs=(vmem, vmem),
    )(packed)


def in_one_kernel(mesh):
    return mesh.shape["grp"] == 2 and mesh.shape["row"] >= 2 * (DEGREE // CY) + 1


def solution(mesh):
    body = on_device
    if in_one_kernel(mesh):
        body = functools.partial(whole_sweeps, mesh.shape["grp"], mesh.shape["row"])
    return jax.shard_map(
        body,
        mesh=mesh,
        in_specs=(
            P(None, ("grp", "row")),
            P(None, ("grp", "row")),
            P(("grp", "row")),
            P(("grp", "row")),
        ),
        out_specs=(P(None, ("grp", "row")), P()),
        check_vma=False,
    )
```

```python
import functools
import math

import jax
import jax.numpy as jnp
import numpy as np
from jax import lax
from jax.experimental import pallas as pl
from jax.experimental.pallas import tpu as pltpu
from jax.sharding import PartitionSpec as P

SWEEPS = 2
DEGREE = 4
CX, CY, CZ = 4, 2, 16
SUB, LANES = 8, 128
MESH = pl.DeviceIdType.MESH
HIGHEST = lax.Precision.HIGHEST


def shifted(block, axis, distance):
    devices = range(lax.axis_size(axis))
    route = [((i - distance) % len(devices), i) for i in devices]
    return lax.ppermute(block, axis, route)


def element_matrix():
    node_ids = np.arange(8)
    corner = np.stack([node_ids % 2, node_ids // 2 % 2, node_ids // 4], axis=1)
    gauss_points = np.array([0.5 - 0.5 / math.sqrt(3.0), 0.5 + 0.5 / math.sqrt(3.0)])
    stiffness = np.zeros((8, 8))
    for q in range(8):
        quad_point = gauss_points[np.array([q % 2, q // 2 % 2, q // 4])]
        values = np.where(corner > 0.5, quad_point, 1.0 - quad_point)
        slopes = np.where(corner > 0.5, 1.0, -1.0)
        gradient = np.stack(
            [
                slopes[:, 0] * values[:, 1] * values[:, 2],
                values[:, 0] * slopes[:, 1] * values[:, 2],
                values[:, 0] * values[:, 1] * slopes[:, 2],
            ],
            axis=1,
        )
        stiffness = stiffness + gradient @ gradient.T / 8.0
    return stiffness


def element_images(window, offsets, weights, stiffness):
    corners = window[:, offsets]
    images = (
        jnp.einsum("ml,rle->rme", stiffness, corners, precision=lax.Precision.HIGHEST) * weights
    )
    return jnp.zeros_like(window).at[:, offsets].add(images)


def on_device(right_side, links, coefs, reaction):
    stiffness = jnp.asarray(element_matrix(), dtype=jnp.float32)
    count = right_side.shape[1]
    groups = lax.axis_size("grp")
    rowcount = lax.axis_size("row")
    group_id = lax.axis_index("grp")
    row_id = lax.axis_index("row")
    total = count * groups * rowcount
    owner = links // count
    slot = links % count
    first = jnp.mod(owner // rowcount - group_id, groups)
    second = jnp.mod(owner % rowcount - row_id, rowcount)
    offsets = (first * 2 + second) * count + slot

    def apply_operator(field):
        above_row = shifted(field, "row", -1)
        upper = shifted(jnp.stack([field, above_row], axis=0), "grp", -1)
        window = jnp.concatenate([field, above_row, upper[0], upper[1]], axis=1)
        summed = element_images(window, offsets, coefs, stiffness)
        back = shifted(
            jnp.stack([summed[:, 2 * count : 3 * count], summed[:, 3 * count :]], axis=0), "grp", 1
        )
        first_col = summed[:, :count] + back[0]
        second_col = summed[:, count : 2 * count] + back[1]
        first_col = first_col + shifted(second_col, "row", 1)
        return first_col + reaction * field

    image = apply_operator(right_side)
    cross, square = lax.psum(
        (jnp.sum(right_side * image, axis=1), jnp.sum(image * image, axis=1)), ("grp", "row")
    )
    theta = square / cross
    upper = (1.5 * theta)[:, None]
    lower = upper / 10.0
    center = (upper + lower) / 2.0
    half = (upper - lower) / 2.0
    sigma = center / half
    solution = jnp.zeros_like(right_side)
    residual = right_side
    history = []
    for sweep in range(SWEEPS):
        start = residual
        correction = jnp.zeros_like(right_side)
        rho_now = 1.0 / sigma
        direction = residual / center
        for step in range(DEGREE):
            correction = correction + direction
            residual = residual - apply_operator(direction)
            if step + 1 < DEGREE:
                rho_next = 1.0 / (2.0 * sigma - rho_now)
                direction = rho_next * rho_now * direction + 2.0 * rho_next / half * residual
                rho_now = rho_next
        change = start - residual
        along, length, begin = lax.psum(
            (
                jnp.sum(start * change, axis=1),
                jnp.sum(change * change, axis=1),
                jnp.sum(start * start, axis=1),
            ),
            ("grp", "row"),
        )
        omega = along / length
        residual = start - omega[:, None] * change
        squares = begin - 2.0 * omega * along + omega * omega * length
        solution = solution + omega[:, None] * correction
        history.append(jnp.sqrt(squares / total))
    return (solution, jnp.stack(history, axis=0))


def next_x(plane):
    return jnp.concatenate([plane[1:], plane[:1]], axis=0)


def last_x(plane):
    return jnp.concatenate([plane[-1:], plane[:-1]], axis=0)


def next_z(plane):
    turned = pltpu.roll(plane, SUB - 1, 1)
    place = lax.broadcasted_iota(jnp.int32, plane.shape, 1)
    return jnp.where(place == SUB - 1, pltpu.roll(turned, LANES // 2, 2), turned)


def last_z(plane):
    turned = pltpu.roll(plane, 1, 1)
    place = lax.broadcasted_iota(jnp.int32, plane.shape, 1)
    return jnp.where(place == 0, pltpu.roll(turned, LANES // 2, 2), turned)


def two_sum(a, b):
    total = a + b
    part = total - a
    return total, (a - (total - part)) + (b - part)


def halves(a):
    scaled = 4097.0 * a
    high = scaled - (scaled - a)
    return high, a - high


def scaled_sum(weights, pairs):
    total = rest = None
    for weight, (value, error) in zip(weights, pairs):
        product = weight * value
        weight_high, weight_low = halves(weight)
        high, low = halves(value)
        lost = ((weight_high * high - product) + weight_high * low + weight_low * high) + weight_low * low
        lost = lost + weight * error
        if total is None:
            total, rest = product, lost
        else:
            total, error = two_sum(total, product)
            rest = rest + (error + lost)
    return total, rest


def chebyshev_weights(theta):
    upper = 1.5 * theta
    lower = upper / 10.0
    center = (upper + lower) / 2.0
    half = (upper - lower) / 2.0
    sigma = center / half
    rho_now = 1.0 / sigma
    direction = [1.0 / center]
    residual = [jnp.ones_like(theta)]
    correction = []
    for step in range(DEGREE):
        size = len(direction)
        correction = [
            direction[k] + correction[k] if k < len(correction) else direction[k]
            for k in range(size)
        ]
        residual = [residual[0]] + [
            residual[k] - direction[k - 1] if k < len(residual) else -direction[k - 1]
            for k in range(1, size + 1)
        ]
        if step + 1 < DEGREE:
            rho_next = 1.0 / (2.0 * sigma - rho_now)
            direction = [
                rho_next * rho_now * direction[k] + 2.0 * rho_next / half * residual[k]
                if k < size
                else 2.0 * rho_next / half * residual[k]
                for k in range(size + 1)
            ]
            rho_now = rho_next
    return correction, [-value for value in residual[1:]]


def kernel(
    groups, rowcount, total,
    right_ref, links_ref, coefs_ref, react_ref,
    packed_ref,
    field, mass, diag, edge_x, edge_y, edge_z, aux,
    power1, power2, power3, power4, grams, sums,
    field_send, field_recv, aux_send, aux_recv, sums_send, sums_recv,
):
    half_reach = DEGREE // CY
    reach = SWEEPS * half_reach
    grp = lax.axis_index("grp")
    row = lax.axis_index("row")
    own = range(reach * CY, reach * CY + CY)
    nrhs = right_ref.shape[0]
    count = right_ref.shape[1]

    def row_at(offset):
        return lax.rem(row + offset + rowcount, rowcount)

    far = sorted(range(-reach, reach + 1), key=lambda o: (abs(o) > half_reach, -abs(o)))
    near = [(o, d) for o in far for d in range(groups)]
    near = [(o, d) for o, d in near if o or d]

    barrier = pltpu.get_barrier_semaphore()
    greeted = 0
    for o in range(1, rowcount):
        pl.semaphore_signal(barrier, inc=1, device_id=(grp, row_at(o)), device_id_type=MESH)
        greeted += 1
    for o, d in near:
        if d:
            peer = (lax.rem(grp + d, groups), row_at(o))
            pl.semaphore_signal(barrier, inc=1, device_id=peer, device_id_type=MESH)
            greeted += 1

    home = (grp * rowcount + row) * count
    slots = jnp.broadcast_to(links_ref[0:1, :] - home, (count, count))
    slot_of = (slots == lax.broadcasted_iota(jnp.int32, (count, count), 0)).astype(jnp.float32)
    order = jnp.transpose(slot_of)
    lanes = lax.broadcasted_iota(jnp.int32, (CX, SUB, LANES), 2)
    low = lanes < LANES // 2
    react = jnp.dot(
        jnp.broadcast_to(react_ref[...], (SUB, count)), slot_of,
        precision=HIGHEST, preferred_element_type=jnp.float32,
    )
    which = lax.broadcasted_iota(jnp.int32, (SUB, count), 0)
    my_aux = reach * groups + grp
    aux[my_aux] = jnp.where(
        which == 0, jnp.broadcast_to(coefs_ref[...], (SUB, count)) * (1.0 / 12.0), react
    )
    twice = jnp.concatenate([right_ref[...], right_ref[...]], axis=0)
    nodes = lax.dot_general(
        order, twice, (((1,), (1,)), ((), ())), precision=HIGHEST,
        preferred_element_type=jnp.float32,
    ).reshape(CX, CY, 2, SUB, LANES)
    for y in range(CY):
        field[reach * CY + y, pl.ds(grp * CX, CX)] = jnp.where(low, nodes[:, y, 0], nodes[:, y, 1])

    pl.semaphore_wait(barrier, greeted)
    aux_copies, field_copies = [], []
    for k, (o, d) in enumerate(near):
        peer = (lax.rem(grp + d, groups), row_at(o))
        copy = pltpu.make_async_remote_copy(
            src_ref=aux.at[my_aux], dst_ref=aux.at[(reach - o) * groups + grp],
            send_sem=aux_send.at[k], recv_sem=aux_recv.at[k], device_id=peer, device_id_type=MESH,
        )
        copy.start()
        aux_copies.append(copy)
    for k, (o, d) in enumerate(near):
        peer = (lax.rem(grp + d, groups), row_at(o))
        copy = pltpu.make_async_remote_copy(
            src_ref=field.at[pl.ds(reach * CY, CY), pl.ds(grp * CX, CX)],
            dst_ref=field.at[pl.ds((reach - o) * CY, CY), pl.ds(grp * CX, CX)],
            send_sem=field_send.at[k], recv_sem=field_recv.at[k], device_id=peer, device_id_type=MESH,
        )
        copy.start()
        field_copies.append(copy)

    blocks = 2 * reach + 1
    planes = blocks * CY
    inner = [abs(o) <= half_reach for o, d in near]
    low_plane, top_plane = half_reach * CY, planes - half_reach * CY

    def expand(begin, end):
        table = aux[begin * groups : end * groups].reshape((end - begin) * groups * SUB, count)
        spare = -table.shape[0] % count
        table = jnp.concatenate([table, jnp.zeros((spare, count), jnp.float32)], axis=0)
        columns = [
            jnp.transpose(table[k : k + count]).reshape(CX, CY, 2, SUB, LANES)
            for k in range(0, table.shape[0], count)
        ]
        for b in range(begin, end):
            for g in range(groups):
                for y in range(CY):
                    for entry, target in ((0, mass), (1, diag)):
                        part, at = divmod(((b - begin) * groups + g) * SUB + entry, count)
                        part = columns[part]
                        first = jnp.broadcast_to(part[:, y, 0, :, at : at + 1], (CX, SUB, LANES))
                        second = jnp.broadcast_to(part[:, y, 1, :, at : at + 1], (CX, SUB, LANES))
                        target[b * CY + y, g * CX : (g + 1) * CX] = jnp.where(low, first, second)

    def edges(begin, end):
        before_xz = before_x = before_z = None
        for y in range(begin, end):
            here = mass[y]
            here_z = here + last_z(here)
            here_x = here + last_x(here)
            here_xz = here_z + last_x(here_z)
            edge_y[y] = here_xz
            if y > begin:
                edge_x[y] = here_z + before_z
                edge_z[y] = here_x + before_x
                diag[y] = diag[y] + 5.0 * (here_xz + before_xz)
            before_xz, before_x, before_z = here_xz, here_x, here_z

    for copy, is_inner in zip(aux_copies, inner):
        if is_inner:
            copy.wait_recv()
    expand(half_reach, blocks - half_reach)
    edges(low_plane, top_plane - 1)

    def apply_operator(source, target, begin, end):
        def gathered(y):
            value = source[y]
            above = next_z(value)
            pair = value + above
            return value, above, pair + next_x(pair)

        last, _, last_sum = gathered(begin - 1)
        value, above, here_sum = gathered(begin)
        last_push = mass[begin - 1] * (last_sum + here_sum)
        for y in range(begin, end):
            following, following_above, following_sum = gathered(y + 1)
            push = mass[y] * (here_sum + following_sum)
            push_y = push + last_push
            push_x = push_y + last_x(push_y)
            result = diag[y] * value - push_x + edge_z[y] * above
            result = result + edge_x[y] * next_x(value) + last_x(edge_x[y] * value)
            result = result + edge_y[y] * following + edge_y[y - 1] * last
            target[y] = result + last_z(edge_z[y] * value - push_x)
            last, last_push = value, push
            value, above, here_sum = following, following_above, following_sum

    def across(products):
        return jnp.sum(jnp.sum(products, axis=0), axis=0, keepdims=True)

    def start_sum(number, slots, rows):
        rows = rows + [jnp.zeros_like(rows[0])] * (slots.shape[1] - len(rows))
        slots[row] = jnp.concatenate(rows, axis=0)
        copies = []
        for o in sorted(range(1, rowcount), key=lambda o: -min(o, rowcount - o)):
            copy = pltpu.make_async_remote_copy(
                src_ref=slots.at[row], dst_ref=slots.at[row],
                send_sem=sums_send.at[number, o - 1], recv_sem=sums_recv.at[number, o - 1],
                device_id=(grp, row_at(o)), device_id_type=MESH,
            )
            copy.start()
            copies.append(copy)
        return copies

    def end_sum(slots, copies):
        for copy in copies:
            copy.wait_recv()
        added, rest = slots[0], jnp.zeros_like(slots[0])
        for k in range(1, rowcount):
            added, error = two_sum(added, slots[k])
            rest = rest + error
        added, error = two_sum(added, pltpu.roll(added, LANES // 2, 1))
        return added, rest + pltpu.roll(rest, LANES // 2, 1) + error

    def spread(line):
        return jnp.broadcast_to(line, (SUB, LANES))

    def combined(weights, powers, y):
        value = weights[0] * powers[0][y]
        for weight, power in zip(weights[1:], powers[1:]):
            value = value + weight * power[y]
        return value

    for copy, is_inner in zip(field_copies, inner):
        if is_inner:
            copy.wait_recv()
    powers = [field, power1, power2, power3, power4]
    for k in range(DEGREE):
        apply_operator(powers[k], powers[k + 1], low_plane + k + 1, top_plane - k - 1)
    pairs = [(j, k) for j in range(DEGREE + 1) for k in range(max(j, 1), DEGREE + 1)]
    products = [
        across(sum(powers[j][y] * powers[k][y] for y in own)) for j, k in pairs
    ]
    bound = start_sum(0, grams, products)
    for copy, is_inner in zip(aux_copies, inner):
        if not is_inner:
            copy.wait_recv()
    expand(0, half_reach)
    expand(blocks - half_reach, blocks)
    edges(0, low_plane + 1)
    edges(top_plane - 2, planes - 1)
    for copy, is_inner in zip(field_copies, inner):
        if not is_inner:
            copy.wait_recv()
    for k in range(DEGREE):
        apply_operator(powers[k], powers[k + 1], k + 1, low_plane + k + 1)
        apply_operator(powers[k], powers[k + 1], top_plane - k - 1, planes - k - 1)

    half_rows = [order.reshape(CX, CY, 2, SUB, count)[:, :, z] for z in range(2)]
    half_rows = [
        jnp.concatenate([part[:, y].reshape(CX * SUB, count) for y in range(CY)], axis=0)
        for part in half_rows
    ]

    def mine(y, value):
        return jnp.where(grp == 0, value[:CX], value[CX:])

    def to_slots(parts):
        stacked = jnp.concatenate([part.reshape(CX * SUB, LANES) for part in parts], axis=0)
        turned = jnp.transpose(stacked)
        return sum(
            jnp.dot(
                turned[z * nrhs : (z + 1) * nrhs], half_rows[z],
                precision=HIGHEST, preferred_element_type=jnp.float32,
            )
            for z in range(2)
        )

    added, rest = end_sum(grams, bound)
    gram = {
        pair: (spread(added[at : at + 1]), spread(rest[at : at + 1])) for at, pair in enumerate(pairs)
    }
    correct, differ = chebyshev_weights(gram[1, 1][0] / gram[0, 1][0])
    along = scaled_sum(differ, [gram[0, k] for k in range(1, DEGREE + 1)])
    length = scaled_sum(
        differ,
        [
            scaled_sum(differ, [gram[min(j, k), max(j, k)] for k in range(1, DEGREE + 1)])
            for j in range(1, DEGREE + 1)
        ],
    )
    omega = (along[0] + along[1]) / (length[0] + length[1])
    corrections = [omega * mine(y, combined(correct, powers[:-1], y)) for y in own]
    for copy in field_copies:
        copy.wait_send()
    steps = [omega * weight for weight in differ]
    for y in range(low_plane, top_plane):
        field[y] = field[y] - combined(steps, powers[1:], y)
    for k in range(DEGREE):
        apply_operator(powers[k], powers[k + 1], low_plane + k + 1, top_plane - k - 1)
    along = length = begin = 0.0
    for y in own:
        change = combined(differ, powers[1:], y)
        along = along + across(field[y] * change)
        length = length + across(change * change)
        begin = begin + across(field[y] * field[y])
    step_sum = start_sum(1, sums, [along, length, begin])
    settled = to_slots(corrections)
    later = to_slots([mine(y, combined(correct, powers[:-1], y)) for y in own])
    added = sum(end_sum(sums, step_sum))
    along, length, begin = (spread(added[k : k + 1]) for k in range(3))
    omega = along / length
    first_rms = jnp.sqrt(begin / total)
    second_rms = jnp.sqrt((begin - 2.0 * omega * along + omega * omega * length) / total)
    packed_ref[pl.ds(nrhs, SUB)] = jnp.where(
        lax.broadcasted_iota(jnp.int32, (SUB, LANES), 0) == 0, first_rms, second_rms
    )
    column = jnp.transpose(jnp.broadcast_to(omega[0:1], (LANES, LANES)))[:nrhs]
    packed_ref[pl.ds(0, nrhs)] = settled + column * later
    for copy in aux_copies + bound + step_sum:
        copy.wait_send()


def unpack(packed_ref, out_ref, rms_ref):
    nrhs = out_ref.shape[0]
    out_ref[...] = packed_ref[:nrhs]
    rms_ref[...] = packed_ref[nrhs : nrhs + SWEEPS, :nrhs]


def whole_sweeps(groups, rowcount, right_side, links, coefs, reaction):
    nrhs, count = right_side.shape
    reach = SWEEPS * (DEGREE // CY)
    planes = (2 * reach + 1) * CY
    window = pltpu.VMEM((planes, groups * CX, SUB, LANES), jnp.float32)
    nears = groups * (2 * reach + 1) - 1
    dma = pltpu.SemaphoreType.DMA
    vmem = pl.BlockSpec(memory_space=pltpu.VMEM)
    packed = pl.pallas_call(
        functools.partial(kernel, groups, rowcount, count * groups * rowcount),
        out_shape=jax.ShapeDtypeStruct((nrhs + SUB, count), jnp.float32),
        in_specs=[vmem] * 4,
        out_specs=vmem,
        scratch_shapes=[
            window, window, window, window, window, window,
            pltpu.VMEM(((2 * reach + 1) * groups, SUB, count), jnp.float32),
            window, window, window, window,
            pltpu.VMEM((rowcount, 2 * SUB, LANES), jnp.float32),
            pltpu.VMEM((rowcount, 4, LANES), jnp.float32),
            dma((nears,)), dma((nears,)), dma((nears,)), dma((nears,)),
            dma((SWEEPS, rowcount - 1)), dma((SWEEPS, rowcount - 1)),
        ],
        compiler_params=pltpu.CompilerParams(collective_id=0, has_side_effects=True),
    )(right_side, links, coefs.reshape(1, count), reaction.reshape(1, count))
    return pl.pallas_call(
        unpack,
        out_shape=(
            jax.ShapeDtypeStruct((nrhs, count), jnp.float32),
            jax.ShapeDtypeStruct((SWEEPS, nrhs), jnp.float32),
        ),
        in_specs=[vmem],
        out_specs=(vmem, vmem),
    )(packed)


def in_one_kernel(mesh):
    return mesh.shape["grp"] == 2 and mesh.shape["row"] >= 2 * SWEEPS * (DEGREE // CY) + 1


def solution(mesh):
    body = on_device
    if in_one_kernel(mesh):
        body = functools.partial(whole_sweeps, mesh.shape["grp"], mesh.shape["row"])
    return jax.shard_map(
        body,
        mesh=mesh,
        in_specs=(
            P(None, ("grp", "row")),
            P(None, ("grp", "row")),
            P(("grp", "row")),
            P(("grp", "row")),
        ),
        out_specs=(P(None, ("grp", "row")), P()),
        check_vma=False,
    )
```
